32 devices in a mesh: dp: 1, ep: 32 (over x, y, z, core).
Axes of the slice: x: 2, y: 2, z: 4, core: 2. Of those that a mesh axis runs over, the one named last changes fastest.
Arguments:
- x: bfloat16 [1, 32, 256, 1792], P('dp', 'ep')
- expert: int32 [1, 32, 256, 8], P('dp', 'ep')
- slot: int32 [1, 32, 256, 8], P('dp', 'ep')
- gate: float32 [1, 32, 256, 8], P('dp', 'ep')
- w_gate: bfloat16 [64, 1792, 2560], P('ep')
- w_up: bfloat16 [64, 1792, 2560], P('ep')
- w_down: bfloat16 [64, 2560, 1792], P('ep')
- s_gate: bfloat16 [1792, 20480], replicated
- s_up: bfloat16 [1792, 20480], replicated
- s_down: bfloat16 [20480, 1792], replicated
Outputs:
- y: bfloat16 [1, 32, 256, 1792], P('dp', 'ep')
All inputs are finite; a program needn't handle non-finite values.
Results may differ from the reference program's by a relative error of at most 0.009.
Values are sent between devices in bfloat16 or wider.
A program may use at most 2 GiB of HBM per device.

```python
import jax
import jax.numpy as jnp

MEMBERS = 32
TOKENS = 256
D = 1792
FF = 2560
TOP = 8
EXPERTS = 64
SHARED_FF = 20480
SLOTS = 5 * TOKENS * TOP // (4 * EXPERTS)


def setup_inputs(seed: int = 0, part: int = 0) -> dict:
    own, k1, k2, k3, k4, k5, k6 = jax.random.split(jax.random.key(seed), 7)
    kx, ke, kl, kg = jax.random.split(jax.random.fold_in(own, part), 4)
    devices = (1, MEMBERS)
    place = jax.random.permutation(kl, jnp.arange(EXPERTS, dtype=jnp.uint32))
    slow = ((EXPERTS + (9 * place) % EXPERTS) << ((9 * place) // EXPERTS)) // EXPERTS
    wait = (jax.random.bits(ke, (*devices, TOKENS, EXPERTS), jnp.uint32) >> 10) * slow
    expert = jnp.argsort(wait, axis=-1)[..., :TOP].astype(jnp.int32)
    chosen = jax.nn.one_hot(expert, EXPERTS, dtype=jnp.int32)
    in_line = jnp.cumsum(chosen.reshape(*devices, TOKENS * TOP, EXPERTS), axis=2) - 1
    slot = jnp.sum(in_line.reshape(chosen.shape) * chosen, axis=-1)

    def one(key, rows, columns):
        return (jax.random.normal(key, (rows, columns), jnp.float32) * rows**-0.5).astype(jnp.bfloat16)

    def weights(key, rows, columns):
        return jax.lax.map(lambda k: one(k, rows, columns), jax.random.split(key, EXPERTS))

    return {
        "x": jax.random.normal(kx, (*devices, TOKENS, D), jnp.float32).astype(jnp.bfloat16),
        "expert": expert,
        "slot": slot,
        "gate": jax.nn.softmax(jax.random.normal(kg, expert.shape, jnp.float32)),
        "w_gate": weights(k1, D, FF),
        "w_up": weights(k2, D, FF),
        "w_down": weights(k3, FF, D),
        "s_gate": one(k4, D, SHARED_FF),
        "s_up": one(k5, D, SHARED_FF),
        "s_down": one(k6, SHARED_FF, D),
    }


def einsum(form, a, b):
    return jnp.einsum(form, a.astype(jnp.float32), b.astype(jnp.float32))


def for_all(x, s_gate, s_up, s_down):
    h = jax.nn.silu(einsum("...d,df->...f", x, s_gate)) * einsum("...d,df->...f", x, s_up)
    return einsum("...f,fd->...d", h.astype(jnp.bfloat16), s_down)


def reference(x, expert, slot, gate, w_gate, w_up, w_down, s_gate, s_up, s_down):
    to_expert = jax.nn.one_hot(expert, EXPERTS, dtype=jnp.bfloat16)
    to_slot = jax.nn.one_hot(slot, SLOTS, dtype=jnp.bfloat16)
    weighted = to_expert * gate[..., None].astype(jnp.bfloat16)
    dispatch = einsum("abtke,abtkc->abtec", to_expert, to_slot).astype(jnp.bfloat16)
    combine = einsum("abtke,abtkc->abtec", weighted, to_slot).astype(jnp.bfloat16)
    z = einsum("abtec,abtd->aebcd", dispatch, x).astype(jnp.bfloat16)
    h = jax.nn.silu(einsum("aebcd,edf->aebcf", z, w_gate))
    h = (h * einsum("aebcd,edf->aebcf", z, w_up)).astype(jnp.bfloat16)
    out = einsum("aebcf,efd->aebcd", h, w_down).astype(jnp.bfloat16)
    y = einsum("abtec,aebcd->abtd", combine, out)
    return (y + for_all(x, s_gate, s_up, s_down)).astype(jnp.bfloat16)
```

```python
import functools

import jax
import jax.numpy as jnp
from jax import lax
from jax.experimental import pallas as pl
from jax.experimental.pallas import tpu as pltpu
from jax.sharding import PartitionSpec as P


ZS = 4
PLANE = 8
PAIRS = ((1, 2), (3, 0))
BACK = ((1, 2), (3,), (0,))
SHARED_TILE = 1024
EXPERT_TILE = 512
VMEM = 60 * 2**20


def dot(form, a, b):
    return jnp.einsum(form, a, b, preferred_element_type=jnp.float32)


def mm(a, b):
    return jnp.dot(a, b, preferred_element_type=jnp.float32)


def shared_kernel(z_ref, x_ref, g_ref, u_ref, d_ref, o_ref):
    h = (jax.nn.silu(mm(x_ref[...], g_ref[...])) * mm(x_ref[...], u_ref[...])).astype(jnp.bfloat16)

    @pl.when(pl.program_id(0) == 0)
    def _():
        o_ref[...] = mm(h, d_ref[...])

    @pl.when(pl.program_id(0) > 0)
    def _():
        o_ref[...] += mm(h, d_ref[...])


def shared_part(z, x, s_gate, s_up, s_down):
    rows, d = x.shape
    tile = SHARED_TILE
    steps = s_gate.shape[1] // (ZS * tile)
    return pl.pallas_call(
        shared_kernel,
        grid_spec=pltpu.PrefetchScalarGridSpec(
            num_scalar_prefetch=1,
            grid=(steps,),
            in_specs=[
                pl.BlockSpec((rows, d), lambda i, z: (0, 0)),
                pl.BlockSpec((d, tile), lambda i, z: (0, i + z[0] * steps)),
                pl.BlockSpec((d, tile), lambda i, z: (0, i + z[0] * steps)),
                pl.BlockSpec((tile, d), lambda i, z: (i + z[0] * steps, 0)),
            ],
            out_specs=pl.BlockSpec((rows, d), lambda i, z: (0, 0)),
        ),
        out_shape=jax.ShapeDtypeStruct((rows, d), jnp.float32),
        compiler_params=pltpu.CompilerParams(vmem_limit_bytes=VMEM, dimension_semantics=("arbitrary",)),
        cost_estimate=pl.CostEstimate(
            flops=6 * rows * d * tile * steps, bytes_accessed=6 * d * tile * steps, transcendentals=rows * tile * steps
        ),
        name="shared",
    )(z.reshape(1), x, s_gate, s_up, s_down)


def expert_kernel(count, *refs):
    v_refs, (g_ref, u_ref, d_ref), o_refs = refs[:count], refs[count : count + 3], refs[count + 3 : -2]
    held, acc = refs[-2:]
    d = held.shape[-1]
    part = held.shape[0] // count
    f = pl.program_id(1)

    @pl.when(f == 0)
    def _():
        for j, v_ref in enumerate(v_refs):
            held[pl.ds(j * part, part)] = v_ref[...].reshape(part, d)

    v = held[...]
    h = (jax.nn.silu(mm(v, g_ref[0])) * mm(v, u_ref[0])).astype(jnp.bfloat16)
    y = mm(h, d_ref[0])

    @pl.when(f == 0)
    def _():
        acc[...] = y

    @pl.when(f > 0)
    def _():
        acc[...] += y

    @pl.when(f == pl.num_programs(1) - 1)
    def _():
        shape = v_refs[0].shape
        for j in range(count):
            out = acc[pl.ds(j * part, part)].astype(jnp.bfloat16).reshape(shape)
            if len(o_refs) == 1:
                o_refs[0][:, :, pl.ds(j * shape[2], shape[2])] = out
            else:
                o_refs[j][...] = out


def experts_of(vs, w_gate, w_up, w_down, joined):
    senders, mine, slots, d = vs[0].shape
    rows = len(vs) * senders * slots
    ff = w_gate.shape[-1]
    tile = EXPERT_TILE
    block = pl.BlockSpec((senders, 1, slots, d), lambda e, f: (0, e, 0, 0))
    outs = 1 if joined else len(vs)
    wide = slots * len(vs) // outs
    return pl.pallas_call(
        functools.partial(expert_kernel, len(vs)),
        grid=(mine, ff // tile),
        in_specs=[block] * len(vs)
        + [
            pl.BlockSpec((1, d, tile), lambda e, f: (e, 0, f)),
            pl.BlockSpec((1, d, tile), lambda e, f: (e, 0, f)),
            pl.BlockSpec((1, tile, d), lambda e, f: (e, f, 0)),
        ],
        out_specs=[pl.BlockSpec((senders, 1, wide, d), lambda e, f: (0, e, 0, 0))] * outs,
        out_shape=[jax.ShapeDtypeStruct((senders, mine, wide, d), jnp.bfloat16)] * outs,
        scratch_shapes=[pltpu.VMEM((rows, d), jnp.bfloat16), pltpu.VMEM((rows, d), jnp.float32)],
        compiler_params=pltpu.CompilerParams(vmem_limit_bytes=VMEM, dimension_semantics=("arbitrary", "arbitrary")),
        cost_estimate=pl.CostEstimate(
            flops=6 * mine * rows * d * ff, bytes_accessed=6 * mine * d * ff, transcendentals=mine * rows * ff
        ),
        name="experts",
    )(*vs, w_gate, w_up, w_down)


def solution(mesh):
    n = mesh.shape["ep"]
    planes = [[16 * x + 8 * y + 2 * z + c for x in (0, 1) for y in (0, 1) for c in (0, 1)] for z in range(ZS)]

    def shift(v, k):
        return lax.ppermute(v, "ep", [(i, i ^ (2 * k)) for i in range(n)])

    def exchange(v):
        return lax.all_to_all(v, "ep", 0, 0, axis_index_groups=planes, tiled=True)

    def body(x, expert, slot, gate, w_gate, w_up, w_down, s_gate, s_up, s_down):
        x, expert, slot, gate = x[0, 0], expert[0, 0], slot[0, 0], gate[0, 0]
        tokens, top = expert.shape
        mine = w_gate.shape[0]
        slots = 5 * tokens * top // (4 * mine * n)
        rows = PLANE * mine * slots
        z = (lax.axis_index("ep") >> 1) & (ZS - 1)

        route = jnp.concatenate([expert, jnp.minimum(slot, slots)], 1).astype(jnp.bfloat16)
        route = jnp.concatenate([route, gate.astype(jnp.bfloat16)], 1).T
        routes = [route] + [shift(route, k) for k in range(1, ZS)]
        xs = [x]
        for k in range(1, ZS):
            xs.append(shift(x, k))

        def place(r):
            e, s = r[:top].astype(jnp.int32), r[top : 2 * top].astype(jnp.int32)
            d, i = e >> 1, e & 1
            p = ((d >> 4) << 2) | (((d >> 3) & 1) << 1) | (d & 1)
            row = (p * mine + i) * slots + s
            return jnp.where((((d >> 1) & (ZS - 1)) == z) & (s < slots), row, -1)

        sent, combine = [], []
        here = lax.broadcasted_iota(jnp.int32, (rows, tokens), 0)
        for k in range(ZS):
            row = place(routes[k])
            g = routes[k][2 * top :].astype(jnp.float32)
            pick = here == row[0]
            weight = jnp.where(here == row[0], g[0], 0.0)
            for j in range(1, top):
                hit = here == row[j]
                pick = pick | hit
                weight = jnp.where(hit, g[j], weight)
            combine.append(weight.astype(jnp.bfloat16))
            sent.append(dot("rt,td->rd", pick.astype(jnp.bfloat16), xs[k]).astype(jnp.bfloat16).reshape(PLANE, mine, slots, -1))

        got = [exchange(v) for v in sent]
        outs = []
        for i, pair in enumerate(PAIRS):
            outs += experts_of([got[k] for k in pair], w_gate, w_up, w_down, joined=i == 0)

        shared = []
        for k in range(ZS):
            shared.append(shared_part(z, xs[k], s_gate, s_up, s_down))
        total = shared[0]
        for i, group in enumerate(BACK):
            v = exchange(outs[i])
            for j, k in enumerate(group):
                back = v[:, :, j * slots : (j + 1) * slots].reshape(rows, -1)
                part = dot("rt,rd->td", combine[k], back)
                if k:
                    part = shift((part + shared[k]).astype(jnp.bfloat16), k)
                    part = part.astype(jnp.float32)
                total = total + part
        return total.astype(jnp.bfloat16)[None, None]

    tok, exp, rep = P("dp", "ep"), P("ep"), P()

    return jax.shard_map(
        body,
        mesh=mesh,
        in_specs=(tok, tok, tok, tok, exp, exp, exp, rep, rep, rep),
        out_specs=tok,
        check_vma=False,
    )
```

```python
import functools

import jax
import jax.numpy as jnp
from jax import lax
from jax.experimental import pallas as pl
from jax.experimental.pallas import tpu as pltpu
from jax.sharding import PartitionSpec as P


ZS = 4
PLANE = 8
PAIRS = ((1, 2), (3, 0))
BACK = ((1, 2), (3,), (0,))
SHARED_TILE = 1024
EXPERT_TILE = 512
DOWN_TILE = 256
SHARED_SPLIT = (0, 5, 9, 13, 16, 20)
VMEM = 67043328


def mm(a, b):
    return jnp.dot(a, b, preferred_element_type=jnp.float32)


def rows_of(route, z, mine, slots):
    top = route.shape[0] // 3
    e, s = route[:top].astype(jnp.int32), route[top : 2 * top].astype(jnp.int32)
    d, i = e >> 1, e & 1
    p = ((d >> 4) << 2) | (((d >> 3) & 1) << 1) | (d & 1)
    return jnp.where((((d >> 1) & (ZS - 1)) == z) & (s < slots), (p * mine + i) * slots + s, -1)


def select_kernel(z_ref, route_ref, x_ref, o_ref):
    senders, mine, slots, _ = o_ref.shape
    count = senders * mine * slots
    row = rows_of(route_ref[...].astype(jnp.float32), z_ref[0], mine, slots)
    here = lax.broadcasted_iota(jnp.int32, (count, row.shape[1]), 0) + pl.program_id(0) * count
    pick = here == row[0:1]
    for j in range(1, row.shape[0]):
        pick = pick | (here == row[j : j + 1])
    pick = jnp.where(pick, 1.0, 0.0).astype(jnp.bfloat16)
    o_ref[...] = mm(pick, x_ref[...]).astype(o_ref.dtype).reshape(o_ref.shape)


def select(z, route, x, mine, slots):
    tokens, d = x.shape
    step = 4
    return pl.pallas_call(
        select_kernel,
        grid_spec=pltpu.PrefetchScalarGridSpec(
            num_scalar_prefetch=1,
            grid=(PLANE // step,),
            in_specs=[
                pl.BlockSpec(route.shape, lambda i, z: (0, 0)),
                pl.BlockSpec((tokens, d), lambda i, z: (0, 0)),
            ],
            out_specs=pl.BlockSpec((step, mine, slots, d), lambda i, z: (i, 0, 0, 0)),
        ),
        out_shape=pltpu.HBM((PLANE, mine, slots, d), jnp.bfloat16),
        compiler_params=pltpu.CompilerParams(vmem_limit_bytes=VMEM, dimension_semantics=("arbitrary",)),
        cost_estimate=pl.CostEstimate(
            flops=2 * PLANE * mine * slots * tokens * d, bytes_accessed=2 * d * (tokens + PLANE * mine * slots), transcendentals=0
        ),
        name="select",
    )(z.reshape(1), route, x)


def combine_kernel(parts, extra, z_ref, v_ref, *refs):
    routes, adds = refs[:parts], refs[parts : parts + extra]
    outs, weight = refs[parts + extra : -1], refs[-1]
    senders, mine, wide, tile = v_ref.shape
    slots = wide // parts
    rows = senders * mine * slots

    @pl.when(pl.program_id(0) == 0)
    def _():
        for j in range(parts):
            route = routes[j][...].astype(jnp.float32)
            row = rows_of(route, z_ref[0], mine, slots)
            top = row.shape[0]
            here = lax.broadcasted_iota(jnp.int32, (rows, row.shape[1]), 0)
            w = jnp.zeros(here.shape, jnp.float32)
            for i in range(top):
                w = jnp.where(here == row[i : i + 1], route[2 * top + i : 2 * top + i + 1], w)
            weight[j] = w.astype(jnp.bfloat16)

    for j in range(parts):
        v = v_ref[:, :, pl.ds(j * slots, slots), :].reshape(rows, tile)
        y = lax.dot_general(weight[j], v, (((0,), (0,)), ((), ())), preferred_element_type=jnp.float32)
        for add in adds:
            y = y + add[...].astype(jnp.float32)
        outs[j][...] = y.astype(jnp.bfloat16)


def combine(z, v, routes, adds):
    parts = len(routes)
    senders, mine, wide, d = v.shape
    tokens = routes[0].shape[1]
    tile = d // 2
    flat = pl.BlockSpec((tokens, tile), lambda i, z: (0, i))
    return pl.pallas_call(
        functools.partial(combine_kernel, parts, len(adds)),
        grid_spec=pltpu.PrefetchScalarGridSpec(
            num_scalar_prefetch=1,
            grid=(d // tile,),
            in_specs=[pl.BlockSpec((senders, mine, wide, tile), lambda i, z: (0, 0, 0, i))]
            + [pl.BlockSpec(routes[0].shape, lambda i, z: (0, 0))] * parts
            + [flat] * len(adds),
            out_specs=[flat] * parts,
            scratch_shapes=[pltpu.VMEM((parts, senders * mine * wide // parts, tokens), jnp.bfloat16)],
        ),
        out_shape=[jax.ShapeDtypeStruct((tokens, d), jnp.bfloat16)] * parts,
        compiler_params=pltpu.CompilerParams(vmem_limit_bytes=VMEM, dimension_semantics=("arbitrary",)),
        cost_estimate=pl.CostEstimate(
            flops=2 * senders * mine * wide * tokens * d, bytes_accessed=2 * d * senders * mine * wide, transcendentals=0
        ),
        name="combine",
    )(z.reshape(1), v, *routes, *adds)


def shared_kernel(started, x_ref, g_ref, u_ref, d_ref, *refs):
    o_ref = refs[-1]
    h = (jax.nn.silu(mm(x_ref[...], g_ref[...])) * mm(x_ref[...], u_ref[...])).astype(jnp.bfloat16)

    @pl.when(pl.program_id(0) == 0)
    def _():
        o_ref[...] = refs[0][...] if started else jnp.zeros_like(o_ref)

    o_ref[...] += mm(h, d_ref[...])


def shared_part(x, s_gate, s_up, s_down, first, last, total):
    rows, d = x.shape
    tile, steps = SHARED_TILE, last - first
    whole = pl.BlockSpec((rows, d), lambda i: (0, 0))
    return pl.pallas_call(
        functools.partial(shared_kernel, total is not None),
        grid=(steps,),
        in_specs=[
            whole,
            pl.BlockSpec((d, tile), lambda i: (0, i + first)),
            pl.BlockSpec((d, tile), lambda i: (0, i + first)),
            pl.BlockSpec((tile, d), lambda i: (i + first, 0)),
        ]
        + [whole] * (total is not None),
        out_specs=whole,
        out_shape=jax.ShapeDtypeStruct((rows, d), jnp.float32),
        compiler_params=pltpu.CompilerParams(vmem_limit_bytes=VMEM, dimension_semantics=("arbitrary",)),
        cost_estimate=pl.CostEstimate(
            flops=6 * rows * d * tile * steps, bytes_accessed=6 * d * tile * steps, transcendentals=rows * tile * steps
        ),
        name="shared",
    )(x, s_gate, s_up, s_down, *([] if total is None else [total]))


def expert_kernel(count, *refs):
    v_refs, (g_ref, u_ref, d_hbm), o_refs = refs[:count], refs[count : count + 3], refs[count + 3 : -4]
    held, h, down, sem = refs[-4:]
    d = held.shape[-1]
    part = held.shape[0] // count
    tile = g_ref.shape[-1]
    e, f = pl.program_id(0), pl.program_id(1)
    fetch = pltpu.make_async_copy(d_hbm.at[e], down, sem)

    @pl.when(f == 0)
    def _():
        fetch.start()
        for j, v_ref in enumerate(v_refs):
            held[pl.ds(j * part, part)] = v_ref[...].reshape(part, d)

    v = held[...]
    out = (jax.nn.silu(mm(v, g_ref[0])) * mm(v, u_ref[0])).astype(jnp.bfloat16)
    h[:, pl.ds(pl.multiple_of(f * tile, tile), tile)] = out

    @pl.when(f == pl.num_programs(1) - 1)
    def _():
        fetch.wait()
        shape = v_refs[0].shape[:-1]
        for c in range(0, d, DOWN_TILE):
            columns = pl.ds(c, DOWN_TILE)
            y = mm(h[...], down[:, columns]).astype(jnp.bfloat16)
            for j in range(count):
                piece = y[j * part : (j + 1) * part].reshape(*shape, DOWN_TILE)
                if len(o_refs) == 1:
                    o_refs[0][:, :, pl.ds(j * shape[2], shape[2]), columns] = piece
                else:
                    o_refs[j][:, :, :, columns] = piece


def experts_of(vs, w_gate, w_up, w_down, joined):
    senders, mine, slots, d = vs[0].shape
    rows = len(vs) * senders * slots
    ff = w_gate.shape[-1]
    tile = EXPERT_TILE
    block = pl.BlockSpec((senders, 1, slots, d), lambda e, f: (0, e, 0, 0))
    outs = 1 if joined else len(vs)
    wide = slots * len(vs) // outs
    return pl.pallas_call(
        functools.partial(expert_kernel, len(vs)),
        grid=(mine, ff // tile),
        in_specs=[block] * len(vs)
        + [
            pl.BlockSpec((1, d, tile), lambda e, f: (e, 0, f)),
            pl.BlockSpec((1, d, tile), lambda e, f: (e, 0, f)),
            pl.BlockSpec(memory_space=pl.ANY),
        ],
        out_specs=[pl.BlockSpec((senders, 1, wide, d), lambda e, f: (0, e, 0, 0))] * outs,
        out_shape=[pltpu.HBM((senders, mine, wide, d), jnp.bfloat16)] * outs,
        scratch_shapes=[
            pltpu.VMEM((rows, d), jnp.bfloat16),
            pltpu.VMEM((rows, ff), jnp.bfloat16),
            pltpu.VMEM((ff, d), jnp.bfloat16),
            pltpu.SemaphoreType.DMA,
        ],
        compiler_params=pltpu.CompilerParams(vmem_limit_bytes=VMEM, dimension_semantics=("arbitrary", "arbitrary")),
        cost_estimate=pl.CostEstimate(
            flops=6 * mine * rows * d * ff, bytes_accessed=6 * mine * d * ff, transcendentals=mine * rows * ff
        ),
        name="experts",
    )(*vs, w_gate, w_up, w_down)


def solution(mesh):
    n = mesh.shape["ep"]
    planes = [[16 * x + 8 * y + 2 * z + c for x in (0, 1) for y in (0, 1) for c in (0, 1)] for z in range(ZS)]

    def shift(v, k):
        return lax.ppermute(v, "ep", [(i, i ^ (2 * k)) for i in range(n)])

    def exchange(v):
        return lax.all_to_all(v, "ep", 0, 0, axis_index_groups=planes, tiled=True)

    def body(x, expert, slot, gate, w_gate, w_up, w_down, s_gate, s_up, s_down):
        x, expert, slot, gate = x[0, 0], expert[0, 0], slot[0, 0], gate[0, 0]
        tokens, top = expert.shape
        mine = w_gate.shape[0]
        slots = 5 * tokens * top // (4 * mine * n)
        z = (lax.axis_index("ep") >> 1) & (ZS - 1)

        route = jnp.concatenate([expert, jnp.minimum(slot, slots)], 1).astype(jnp.bfloat16)
        route = jnp.concatenate([route, gate.astype(jnp.bfloat16)], 1).T
        routes, xs = [route], [x]
        for k in range(1, ZS):
            routes.append(shift(route, k))
            xs.append(shift(x, k))

        sent = []
        for k in range(ZS):
            sent.append(select(z, routes[k], xs[k], mine, slots))
        got = [exchange(v) for v in sent]
        outs = []
        for i, pair in enumerate(PAIRS):
            outs += experts_of([got[k] for k in pair], w_gate, w_up, w_down, joined=i == 0)

        shared = None
        for first, last in zip(SHARED_SPLIT, SHARED_SPLIT[1:]):
            shared = shared_part(x, s_gate, s_up, s_down, first, last, shared)

        arrived = []
        for i, group in enumerate(BACK):
            v = exchange(outs[i])
            parts = combine(z, v, [routes[k] for k in group], () if any(group) else (shared, *arrived))
            for k, part in zip(group, parts):
                if k:
                    arrived.append(shift(part, k))
        return parts[0][None, None]

    tok, exp, rep = P("dp", "ep"), P("ep"), P()

    return jax.shard_map(
        body,
        mesh=mesh,
        in_specs=(tok, tok, tok, tok, exp, exp, exp, rep, rep, rep),
        out_specs=tok,
        check_vma=False,
    )
```

```python
import functools

import jax
import jax.numpy as jnp
from jax import lax
from jax.experimental import pallas as pl
from jax.experimental.pallas import tpu as pltpu
from jax.sharding import PartitionSpec as P


ZS = 4
PLANE = 8
PAIRS = ((1, 2), (3, 0))
BACK = ((1, 2), (3,), (0,))
SHARED_TILE = 1024
EXPERT_TILE = 512
DOWN_TILE = 256
SHARED_SPLIT = (0, 5, 9, 13, 16, 20)
VMEM = 67043328


def mm(a, b):
    return jnp.dot(a, b, preferred_element_type=jnp.float32)


def rows_of(route, z, mine, slots):
    top = route.shape[0] // 3
    e, s = route[:top].astype(jnp.int32), route[top : 2 * top].astype(jnp.int32)
    d, i = e >> 1, e & 1
    p = ((d >> 4) << 2) | (((d >> 3) & 1) << 1) | (d & 1)
    return jnp.where((((d >> 1) & (ZS - 1)) == z) & (s < slots), (p * mine + i) * slots + s, -1)


def select_kernel(z_ref, route_ref, x_ref, o_ref):
    senders, mine, slots, _ = o_ref.shape
    count = senders * mine * slots
    row = rows_of(route_ref[...].astype(jnp.float32), z_ref[0], mine, slots)
    here = lax.broadcasted_iota(jnp.int32, (count, row.shape[1]), 0) + pl.program_id(0) * count
    pick = here == row[0:1]
    for j in range(1, row.shape[0]):
        pick = pick | (here == row[j : j + 1])
    pick = jnp.where(pick, 1.0, 0.0).astype(jnp.bfloat16)
    o_ref[...] = mm(pick, x_ref[...]).astype(o_ref.dtype).reshape(o_ref.shape)


def select(z, route, x, mine, slots):
    tokens, d = x.shape
    step = 4
    return pl.pallas_call(
        select_kernel,
        grid_spec=pltpu.PrefetchScalarGridSpec(
            num_scalar_prefetch=1,
            grid=(PLANE // step,),
            in_specs=[
                pl.BlockSpec(route.shape, lambda i, z: (0, 0)),
                pl.BlockSpec((tokens, d), lambda i, z: (0, 0)),
            ],
            out_specs=pl.BlockSpec((step, mine, slots, d), lambda i, z: (i, 0, 0, 0)),
        ),
        out_shape=pltpu.HBM((PLANE, mine, slots, d), jnp.bfloat16),
        compiler_params=pltpu.CompilerParams(vmem_limit_bytes=VMEM, dimension_semantics=("arbitrary",)),
        cost_estimate=pl.CostEstimate(
            flops=2 * PLANE * mine * slots * tokens * d, bytes_accessed=2 * d * (tokens + PLANE * mine * slots), transcendentals=0
        ),
        name="select",
    )(z.reshape(1), route, x)


def combine_kernel(parts, extra, z_ref, v_ref, *refs):
    routes, adds = refs[:parts], refs[parts : parts + extra]
    outs, weight = refs[parts + extra : -1], refs[-1]
    senders, mine, wide, tile = v_ref.shape
    slots = wide // parts
    rows = senders * mine * slots

    @pl.when(pl.program_id(0) == 0)
    def _():
        for j in range(parts):
            route = routes[j][...].astype(jnp.float32)
            row = rows_of(route, z_ref[0], mine, slots)
            top = row.shape[0]
            here = lax.broadcasted_iota(jnp.int32, (rows, row.shape[1]), 0)
            w = jnp.zeros(here.shape, jnp.float32)
            for i in range(top):
                w = jnp.where(here == row[i : i + 1], route[2 * top + i : 2 * top + i + 1], w)
            weight[j] = w.astype(jnp.bfloat16)

    for j in range(parts):
        v = v_ref[:, :, pl.ds(j * slots, slots), :].reshape(rows, tile)
        y = lax.dot_general(weight[j], v, (((0,), (0,)), ((), ())), preferred_element_type=jnp.float32)
        for add in adds:
            y = y + add[...].astype(jnp.float32)
        outs[j][...] = y.astype(jnp.bfloat16)


def combine(z, v, routes, adds):
    parts = len(routes)
    senders, mine, wide, d = v.shape
    tokens = routes[0].shape[1]
    tile = d // 2
    flat = pl.BlockSpec((tokens, tile), lambda i, z: (0, i))
    return pl.pallas_call(
        functools.partial(combine_kernel, parts, len(adds)),
        grid_spec=pltpu.PrefetchScalarGridSpec(
            num_scalar_prefetch=1,
            grid=(d // tile,),
            in_specs=[pl.BlockSpec((senders, mine, wide, tile), lambda i, z: (0, 0, 0, i))]
            + [pl.BlockSpec(routes[0].shape, lambda i, z: (0, 0))] * parts
            + [flat] * len(adds),
            out_specs=[flat] * parts,
            scratch_shapes=[pltpu.VMEM((parts, senders * mine * wide // parts, tokens), jnp.bfloat16)],
        ),
        out_shape=[jax.ShapeDtypeStruct((tokens, d), jnp.bfloat16)] * parts,
        compiler_params=pltpu.CompilerParams(vmem_limit_bytes=VMEM, dimension_semantics=("arbitrary",)),
        cost_estimate=pl.CostEstimate(
            flops=2 * senders * mine * wide * tokens * d, bytes_accessed=2 * d * senders * mine * wide, transcendentals=0
        ),
        name="combine",
    )(z.reshape(1), v, *routes, *adds)


def shared_kernel(started, x_ref, g_ref, u_ref, d_ref, *refs):
    o_ref = refs[-1]
    h = (jax.nn.silu(mm(x_ref[...], g_ref[...])) * mm(x_ref[...], u_ref[...])).astype(jnp.bfloat16)

    @pl.when(pl.program_id(0) == 0)
    def _():
        o_ref[...] = refs[0][...] if started else jnp.zeros_like(o_ref)

    o_ref[...] += mm(h, d_ref[...])


def shared_part(x, s_gate, s_up, s_down, first, last, total):
    rows, d = x.shape
    tile, steps = SHARED_TILE, last - first
    whole = pl.BlockSpec((rows, d), lambda i: (0, 0))
    return pl.pallas_call(
        functools.partial(shared_kernel, total is not None),
        grid=(steps,),
        in_specs=[
            whole,
            pl.BlockSpec((d, tile), lambda i: (0, i + first)),
            pl.BlockSpec((d, tile), lambda i: (0, i + first)),
            pl.BlockSpec((tile, d), lambda i: (i + first, 0)),
        ]
        + [whole] * (total is not None),
        out_specs=whole,
        out_shape=jax.ShapeDtypeStruct((rows, d), jnp.float32),
        compiler_params=pltpu.CompilerParams(vmem_limit_bytes=VMEM, dimension_semantics=("arbitrary",)),
        cost_estimate=pl.CostEstimate(
            flops=6 * rows * d * tile * steps, bytes_accessed=6 * d * tile * steps, transcendentals=rows * tile * steps
        ),
        name="shared",
    )(x, s_gate, s_up, s_down, *([] if total is None else [total]))


def expert_kernel(count, *refs):
    v_refs, (g_ref, u_ref, d_hbm), o_refs = refs[:count], refs[count : count + 3], refs[count + 3 : -4]
    held, h, down, sem = refs[-4:]
    d = held.shape[-1]
    part = held.shape[0] // count
    tile = g_ref.shape[-1]
    e, f = pl.program_id(0), pl.program_id(1)
    fetch = pltpu.make_async_copy(d_hbm.at[e], down, sem)

    @pl.when(f == 0)
    def _():
        fetch.start()
        for j, v_ref in enumerate(v_refs):
            held[pl.ds(j * part, part)] = v_ref[...].reshape(part, d)

    v = held[...]
    out = (jax.nn.silu(mm(v, g_ref[0])) * mm(v, u_ref[0])).astype(jnp.bfloat16)
    h[:, pl.ds(pl.multiple_of(f * tile, tile), tile)] = out

    @pl.when(f == pl.num_programs(1) - 1)
    def _():
        fetch.wait()
        shape = v_refs[0].shape[:-1]
        for c in range(0, d, DOWN_TILE):
            columns = pl.ds(c, DOWN_TILE)
            y = mm(h[...], down[:, columns]).astype(jnp.bfloat16)
            for j in range(count):
                piece = y[j * part : (j + 1) * part].reshape(*shape, DOWN_TILE)
                if len(o_refs) == 1:
                    o_refs[0][:, :, pl.ds(j * shape[2], shape[2]), columns] = piece
                else:
                    o_refs[j][:, :, :, columns] = piece


def experts_of(vs, w_gate, w_up, w_down, joined):
    senders, mine, slots, d = vs[0].shape
    rows = len(vs) * senders * slots
    ff = w_gate.shape[-1]
    tile = EXPERT_TILE
    block = pl.BlockSpec((senders, 1, slots, d), lambda e, f: (0, e, 0, 0))
    outs = 1 if joined else len(vs)
    wide = slots * len(vs) // outs
    return pl.pallas_call(
        functools.partial(expert_kernel, len(vs)),
        grid=(mine, ff // tile),
        in_specs=[block] * len(vs)
        + [
            pl.BlockSpec((1, d, tile), lambda e, f: (e, 0, f)),
            pl.BlockSpec((1, d, tile), lambda e, f: (e, 0, f)),
            pl.BlockSpec(memory_space=pl.ANY),
        ],
        out_specs=[pl.BlockSpec((senders, 1, wide, d), lambda e, f: (0, e, 0, 0))] * outs,
        out_shape=[pltpu.HBM((senders, mine, wide, d), jnp.bfloat16)] * outs,
        scratch_shapes=[
            pltpu.VMEM((rows, d), jnp.bfloat16),
            pltpu.VMEM((rows, ff), jnp.bfloat16),
            pltpu.VMEM((ff, d), jnp.bfloat16),
            pltpu.SemaphoreType.DMA,
        ],
        compiler_params=pltpu.CompilerParams(vmem_limit_bytes=VMEM, dimension_semantics=("arbitrary", "arbitrary")),
        cost_estimate=pl.CostEstimate(
            flops=6 * mine * rows * d * ff, bytes_accessed=6 * mine * d * ff, transcendentals=mine * rows * ff
        ),
        name="experts",
    )(*vs, w_gate, w_up, w_down)


def solution(mesh):
    n = mesh.shape["ep"]
    planes = [[16 * x + 8 * y + 2 * z + c for x in (0, 1) for y in (0, 1) for c in (0, 1)] for z in range(ZS)]

    def shift(v, k):
        return lax.ppermute(v, "ep", [(i, i ^ (2 * k)) for i in range(n)])

    def exchange(v):
        return lax.all_to_all(v, "ep", 0, 0, axis_index_groups=planes, tiled=True)

    def body(x, expert, slot, gate, w_gate, w_up, w_down, s_gate, s_up, s_down):
        x, expert, slot, gate = x[0, 0], expert[0, 0], slot[0, 0], gate[0, 0]
        tokens, top = expert.shape
        mine = w_gate.shape[0]
        slots = 5 * tokens * top // (4 * mine * n)
        z = (lax.axis_index("ep") >> 1) & (ZS - 1)

        route = jnp.concatenate([expert, jnp.minimum(slot, slots)], 1).astype(jnp.bfloat16)
        route = jnp.concatenate([route, gate.astype(jnp.bfloat16)], 1).T
        routes, xs = [route], [x]
        for k in range(1, ZS):
            routes.append(shift(route, k))
            xs.append(shift(x, k))

        sent = []
        for k in range(ZS):
            sent.append(select(z, routes[k], xs[k], mine, slots))
        got = [exchange(v) for v in sent]
        outs = []
        for i, pair in enumerate(PAIRS):
            outs += experts_of([got[k] for k in pair], w_gate, w_up, w_down, joined=i == 0)

        shared = None
        for first, last in zip(SHARED_SPLIT, SHARED_SPLIT[1:]):
            shared = shared_part(x, s_gate, s_up, s_down, first, last, shared)

        arrived = []
        for i, group in enumerate(BACK):
            v = exchange(outs[i])
            adds = (shared, *arrived) if group == (0,) else (relayed,) if group == (3,) else ()
            parts = combine(z, v, [routes[k] for k in group], adds)
            for k, part in zip(group, parts):
                if k == 2:
                    relayed = shift(part, 1)
                elif k:
                    arrived.append(shift(part, k))
        return parts[0][None, None]

    tok, exp, rep = P("dp", "ep"), P("ep"), P()

    return jax.shard_map(
        body,
        mesh=mesh,
        in_specs=(tok, tok, tok, tok, exp, exp, exp, rep, rep, rep),
        out_specs=tok,
        check_vma=False,
    )
```
